64 devices in a mesh: dp: 4 (over x, y), cp: 16 (over z, core).
Axes of the slice: x: 2, y: 2, z: 8, core: 2. Of those that a mesh axis runs over, the one named last changes fastest.
The devices are a block of a 4x4x8 slice.
Arguments:
- query: bfloat16 [12, 768, 22, 128], P('dp', 'cp'), parts along dimension 0
- key: bfloat16 [12, 768, 128], P('dp', 'cp'), parts along dimension 0
- value: bfloat16 [12, 768, 128], P('dp', 'cp'), parts along dimension 0
- positions: int32 [3072], P(('dp', 'cp')), parts along dimension 0
- grad_out: bfloat16 [12, 768, 22, 128], P('dp', 'cp'), parts along dimension 0
Outputs:
- output 1: bfloat16 [12, 768, 22, 128], P('dp', 'cp'), parts along dimension 0
- output 2: bfloat16 [12, 768, 22, 128], P('dp', 'cp'), parts along dimension 0
- output 3: bfloat16 [12, 768, 128], P('dp', 'cp'), parts along dimension 0
- output 4: bfloat16 [12, 768, 128], P('dp', 'cp'), parts along dimension 0
There are 4 independent parts. The reference program is written for one: setup_inputs(seed, part) draws one part's arguments, and reference() takes and returns one part's arrays. A program takes and returns all parts, laid end to end along the dimension named above; each array names one.
All inputs are finite; a program needn't handle non-finite values.
Results may differ from the reference program's by a relative error of at most 0.00821643.
Values are sent between devices in bfloat16 or wider.
A program may use at most 768 MiB of HBM per device.

```python
import jax
import jax.numpy as jnp
from jax import lax

BATCH = 3
SEQ = 768
HEADS = 22
HEAD = 128
QROWS = 8
ROPE_BASE = 10000


def setup_inputs(seed: int = 0, part: int = 0) -> dict:
    part_key = jax.random.fold_in(jax.random.key(seed), part)
    rng_keys = jax.random.split(part_key, 6)
    query = jax.random.normal(rng_keys[0], (BATCH, SEQ, HEADS, HEAD), jnp.float32)
    key = jax.random.normal(rng_keys[1], (BATCH, SEQ, HEAD), jnp.float32)
    value = jax.random.normal(rng_keys[2], (BATCH, SEQ, HEAD), jnp.float32)
    start = jax.random.randint(rng_keys[3], (), 0, 256)
    increments = jax.random.randint(rng_keys[4], (SEQ,), 0, 2)
    positions = (start + jnp.cumsum(increments)).astype(jnp.int32)
    grad_out = jax.random.normal(rng_keys[5], (BATCH, SEQ, HEADS, HEAD), jnp.float32)
    return {'query': query.astype(jnp.bfloat16), 'key': key.astype(jnp.bfloat16), 'value': value.astype(jnp.bfloat16), 'positions': positions, 'grad_out': grad_out.astype(jnp.bfloat16)}


def rope_tables(positions):
    half_dim = HEAD // 2
    inv_freq = jnp.power(jnp.float32(ROPE_BASE), -2.0 * jnp.arange(half_dim, dtype=jnp.float32) / HEAD)
    angles = positions.astype(jnp.float32)[..., None] * inv_freq
    angles = jnp.concatenate([angles, angles], axis=-1)
    return jnp.cos(angles), jnp.sin(angles)


def rotate(values, cos_tab, sin_tab):
    half_dim = values.shape[-1] // 2
    turned = jnp.concatenate([-values[..., half_dim:], values[..., :half_dim]], axis=-1)
    return values * cos_tab + turned * sin_tab


def reference(query, key, value, positions, grad_out):
    cos_tab, sin_tab = rope_tables(positions)
    cos_q = cos_tab[None, :, None, :]
    sin_q = sin_tab[None, :, None, :]
    query_rot = rotate(query.astype(jnp.float32), cos_q, sin_q).astype(jnp.bfloat16)
    key_rot = rotate(key.astype(jnp.float32), cos_tab[None], sin_tab[None]).astype(jnp.bfloat16)
    scale = HEAD ** -0.5
    key_f = key_rot.astype(jnp.float32)
    value_f = value.astype(jnp.float32)
    key_idx = jnp.arange(SEQ)
    block_count = SEQ // QROWS
    query_blocks = query_rot.reshape(BATCH, block_count, QROWS, HEADS, HEAD).transpose(1, 0, 2, 3, 4)
    grad_blocks = grad_out.reshape(BATCH, block_count, QROWS, HEADS, HEAD).transpose(1, 0, 2, 3, 4)

    def one_block(carry, block):
        dkey_acc, dvalue_acc = carry
        query_blk, grad_blk, block_idx = block
        query_f = query_blk.astype(jnp.float32)
        grad_f = grad_blk.astype(jnp.float32)
        query_idx = block_idx * QROWS + jnp.arange(QROWS)
        causal_mask = (key_idx[None, :] <= query_idx[:, None])[None, :, None, :]
        scores = jnp.where(causal_mask, jnp.einsum('bqhd,bkd->bqhk', query_f, key_f) * scale, -jnp.inf)
        row_max = jnp.max(scores, axis=-1, keepdims=True)
        weights = jnp.exp(scores - row_max)
        row_sum = jnp.sum(weights, axis=-1, keepdims=True)
        attn_f = jnp.einsum('bqhk,bkd->bqhd', weights.astype(jnp.bfloat16).astype(jnp.float32), value_f) / row_sum
        attn_blk = attn_f.astype(jnp.bfloat16)
        probs_f = jnp.exp(scores - (row_max + jnp.log(row_sum)))
        delta = jnp.sum(grad_f * attn_blk.astype(jnp.float32), axis=-1, keepdims=True)
        dprobs = jnp.einsum('bqhd,bkd->bqhk', grad_f, value_f)
        dscore = (probs_f * (dprobs - delta)).astype(jnp.bfloat16).astype(jnp.float32)
        dquery_blk = jnp.einsum('bqhk,bkd->bqhd', dscore, key_f) * scale
        dkey_acc = dkey_acc + jnp.einsum('bqhk,bqhd->bkd', dscore, query_f) * scale
        dvalue_acc = dvalue_acc + jnp.einsum('bqhk,bqhd->bkd', probs_f.astype(jnp.bfloat16).astype(jnp.float32), grad_f)
        return (dkey_acc, dvalue_acc), (attn_blk, dquery_blk)

    zero_kv = jnp.zeros((BATCH, SEQ, HEAD), jnp.float32)
    sums, outs = lax.scan(one_block, (zero_kv, zero_kv), (query_blocks, grad_blocks, jnp.arange(block_count)))
    attn_out = outs[0].transpose(1, 0, 2, 3, 4).reshape(BATCH, SEQ, HEADS, HEAD)
    dquery_rot = outs[1].transpose(1, 0, 2, 3, 4).reshape(BATCH, SEQ, HEADS, HEAD)
    grad_query = rotate(dquery_rot, cos_q, -sin_q).astype(jnp.bfloat16)
    grad_key = rotate(sums[0], cos_tab[None], -sin_tab[None]).astype(jnp.bfloat16)
    grad_value = sums[1].astype(jnp.bfloat16)
    return (attn_out, grad_query, grad_key, grad_value)
```

```python
import functools

import jax
import jax.numpy as jnp
from jax import lax
from jax.experimental import pallas as pl
from jax.experimental.pallas import tpu as pltpu
from jax.sharding import PartitionSpec as P

ROPE_BASE = 10000
LOG2E = 1.4426950408889634
TILE_TOKENS = 8


def rope_tables(positions, head):
    half_dim = head // 2
    inv_freq = jnp.power(jnp.float32(ROPE_BASE), -2.0 * jnp.arange(half_dim, dtype=jnp.float32) / head)
    angles = positions.astype(jnp.float32)[..., None] * inv_freq
    angles = jnp.concatenate([angles, angles], axis=-1)
    return jnp.cos(angles), jnp.sin(angles)


def compute_kernel(pad_heads, scale, q_ref, do_ref, kv_ref, cos_ref, sin_ref, out_ref, dq_ref, part_ref, qn, don, padf, p_buf, ds_buf):
    batch, blk, heads, head = q_ref.shape
    keys = kv_ref.shape[2]
    rows = blk * pad_heads
    tile = TILE_TOKENS * pad_heads
    me = lax.axis_index('cp')
    padf[:, heads:, :] = jnp.zeros((blk, pad_heads - heads, head), jnp.float32)
    cos = cos_ref[...][:, None, :]
    sin = sin_ref[...][:, None, :]

    def prep(b, carry):
        padf[:, :heads, :] = q_ref[b].astype(jnp.float32)
        x = padf[...]
        turned = pltpu.roll(x.reshape(rows, head), head // 2, 1).reshape(blk, pad_heads, head)
        qn[b] = (x * cos + turned * sin).reshape(rows, head).astype(jnp.bfloat16)
        padf[:, :heads, :] = do_ref[b].astype(jnp.float32)
        don[b] = padf[...].reshape(rows, head).astype(jnp.bfloat16)
        return carry

    lax.fori_loop(0, batch, prep, 0)

    def attend(step, carry):
        b = step // (blk // TILE_TOKENS)
        i = step % (blk // TILE_TOKENS)
        row0 = pl.multiple_of(i * tile, tile)
        q_t = qn[b, pl.ds(row0, tile), :]
        do_t = don[b, pl.ds(row0, tile), :]
        k_all = kv_ref[b, 0]
        v_all = kv_ref[b, 1]
        nt = (((1,), (1,)), ((), ()))
        s = lax.dot_general(q_t, k_all, nt, preferred_element_type=jnp.float32)
        tok = lax.broadcasted_iota(jnp.int32, (TILE_TOKENS, pad_heads, 1), 0).reshape(tile, 1) + (me * blk + i * TILE_TOKENS)
        col = lax.broadcasted_iota(jnp.int32, (tile, keys), 1)
        s = jnp.where(col <= tok, s, -jnp.inf)
        m = jnp.max(s, axis=1, keepdims=True)
        e = jnp.exp2((s - m) * (scale * LOG2E))
        inv_l = 1.0 / jnp.sum(e, axis=1, keepdims=True)
        o = jnp.dot(e.astype(jnp.bfloat16), v_all, preferred_element_type=jnp.float32) * inv_l
        ob = o.astype(jnp.bfloat16)
        of = ob.astype(jnp.float32)
        out_ref[b, pl.ds(i * TILE_TOKENS, TILE_TOKENS)] = of.reshape(TILE_TOKENS, pad_heads, head)[:, :heads, :].astype(jnp.bfloat16)
        delta = jnp.sum(do_t.astype(jnp.float32) * of, axis=1, keepdims=True)
        dp = lax.dot_general(do_t, v_all, nt, preferred_element_type=jnp.float32)
        p = e * inv_l
        p_buf[b, pl.ds(row0, tile), :] = p.astype(jnp.bfloat16)
        ds_buf[b, pl.ds(row0, tile), :] = (p * (dp - delta)).astype(jnp.bfloat16)
        return carry

    def key_grads(b):
        tn = (((0,), (0,)), ((), ()))
        dkt = lax.dot_general(qn[b], ds_buf[b], tn, preferred_element_type=jnp.float32)
        part_ref[b, 0] = dkt.T * scale
        dvt = lax.dot_general(don[b], p_buf[b], tn, preferred_element_type=jnp.float32)
        part_ref[b, 1] = dvt.T

    def query_grads(step, carry):
        b = step // (blk // TILE_TOKENS)
        i = step % (blk // TILE_TOKENS)
        row0 = pl.multiple_of(i * tile, tile)
        g = jnp.dot(ds_buf[b, pl.ds(row0, tile), :], kv_ref[b, 0], preferred_element_type=jnp.float32) * scale
        turned = pltpu.roll(g, head // 2, 1).reshape(TILE_TOKENS, pad_heads, head)
        cos_t = cos_ref[pl.ds(i * TILE_TOKENS, TILE_TOKENS), :][:, None, :]
        sin_t = sin_ref[pl.ds(i * TILE_TOKENS, TILE_TOKENS), :][:, None, :]
        g = g.reshape(TILE_TOKENS, pad_heads, head) * cos_t - turned * sin_t
        dq_ref[b, pl.ds(i * TILE_TOKENS, TILE_TOKENS)] = g[:, :heads, :].astype(jnp.bfloat16)
        return carry

    tiles = blk // TILE_TOKENS

    def one_batch(b, carry):
        lax.fori_loop(b * tiles, (b + 1) * tiles, attend, 0)
        key_grads(b)
        lax.fori_loop(b * tiles, (b + 1) * tiles, query_grads, 0)
        return carry

    lax.fori_loop(0, batch, one_batch, 0)


def solution(mesh):
    query_spec = P('dp', 'cp', None, None)
    kv_spec = P('dp', 'cp', None)
    pos_spec = P(('dp', 'cp'))
    cp_size = mesh.shape['cp']

    def per_device(query, key, value, positions, grad_out):
        batch, blk, heads, head = query.shape
        scale = head ** -0.5
        pad_heads = -(-heads // 8) * 8
        rows = blk * pad_heads
        keys = cp_size * blk
        cos_tab, sin_tab = rope_tables(positions, head)
        sin_signed = jnp.where(jnp.arange(head) < head // 2, -sin_tab, sin_tab)
        kf = key.astype(jnp.float32)
        turned = jnp.roll(kf, head // 2, axis=-1)
        key_rot = (kf * cos_tab[None] + turned * sin_signed[None]).astype(jnp.bfloat16)
        kv = lax.all_gather(jnp.stack([key_rot, value], axis=1), 'cp', axis=2, tiled=True)
        vm = pl.BlockSpec(memory_space=pltpu.VMEM)
        attn, dq, part = pl.pallas_call(
            functools.partial(compute_kernel, pad_heads, scale),
            out_shape=(
                jax.ShapeDtypeStruct(query.shape, jnp.bfloat16),
                jax.ShapeDtypeStruct(query.shape, jnp.bfloat16),
                jax.ShapeDtypeStruct((batch, 2, keys, head), jnp.float32),
            ),
            in_specs=[vm] * 5,
            out_specs=(vm, vm, vm),
            scratch_shapes=[
                pltpu.VMEM((batch, rows, head), jnp.bfloat16),
                pltpu.VMEM((batch, rows, head), jnp.bfloat16),
                pltpu.VMEM((blk, pad_heads, head), jnp.float32),
                pltpu.VMEM((batch, rows, keys), jnp.bfloat16),
                pltpu.VMEM((batch, rows, keys), jnp.bfloat16),
            ],
            compiler_params=pltpu.CompilerParams(vmem_limit_bytes=60 * 2**20),
        )(query, grad_out, kv, cos_tab, sin_signed)
        home = lax.psum_scatter(part, 'cp', scatter_dimension=2, tiled=True)
        gk = home[:, 0]
        gk = gk * cos_tab[None] - jnp.roll(gk, head // 2, axis=-1) * sin_signed[None]
        return attn, dq, gk.astype(jnp.bfloat16), home[:, 1].astype(jnp.bfloat16)

    return jax.shard_map(per_device, mesh=mesh, in_specs=(query_spec, kv_spec, kv_spec, pos_spec, query_spec), out_specs=(query_spec, query_spec, kv_spec, kv_spec), check_vma=False)
```
